64 devices in a mesh: dp: 4 (over x, y), ep: 16 (over z, core).
Axes of the slice: x: 2, y: 2, z: 8, core: 2. Of those that a mesh axis runs over, the one named last changes fastest.
The devices are a block of a 4x4x8 slice.
Arguments:
- tokens: bfloat16 [2, 64, 512, 1536], P(None, ('dp', 'ep')), parts along dimension 1
- expert_ids: int32 [2, 32768, 6], P(None, ('dp', 'ep')), parts along dimension 1
- route_weights: float32 [2, 32768, 6], P(None, ('dp', 'ep')), parts along dimension 1
- attn_norm: bfloat16 [1536], replicated
- w_query: bfloat16 [1536, 12, 128], replicated
- w_key: bfloat16 [1536, 12, 128], replicated
- w_value: bfloat16 [1536, 12, 128], replicated
- w_out: bfloat16 [12, 128, 1536], replicated
- ffn_norm: bfloat16 [1536], replicated
- w_gate: bfloat16 [64, 1536, 512], P('ep')
- w_up: bfloat16 [64, 1536, 512], P('ep')
- w_down: bfloat16 [64, 512, 1536], P('ep')
- shared_gate: bfloat16 [1536, 1024], replicated
- shared_up: bfloat16 [1536, 1024], replicated
- shared_down: bfloat16 [1024, 1536], replicated
Outputs:
- output: bfloat16 [2, 64, 512, 1536], P(None, ('dp', 'ep')), parts along dimension 1
There are 4 independent parts. The reference program is written for one: setup_inputs(seed, part) draws one part's arguments, and reference() takes and returns one part's arrays. A program takes and returns all parts, laid end to end along the dimension named above; an argument that names none is the same for every part.
All inputs are finite; a program needn't handle non-finite values.
Results may differ from the reference program's by a relative error of at most 0.00977376.
Values are sent between devices in bfloat16 or wider.
A program may use at most 768 MiB of HBM per device.

```python
import jax
import jax.numpy as jnp
import numpy as np
from jax import lax

TOKENS = 512
SEQ = 512
D_MODEL = 1536
HEADS = 12
HEAD_DIM = 128
EXPERTS = 64
TOP = 6
FF = 512
SHARED_FF = 1024
GROUP = 16
CAPACITY = 96
NORM_EPS = 1e-6


def load_profile():
    total_rows = TOKENS * TOP
    rest_rows = total_rows - CAPACITY
    weight_list = [3 * (EXPERTS - 1) - 2 * rank_pos for rank_pos in range(EXPERTS - 1)]
    weight_sum = sum(weight_list)
    count_list = [rest_rows * weight_val // weight_sum for weight_val in weight_list]
    extra_units = rest_rows - sum(count_list)
    count_list = [count_val + (1 if rank_pos < extra_units else 0) for rank_pos, count_val in enumerate(count_list)]
    return [CAPACITY] + count_list


def draw_routing(base_key):
    rank_ids = np.repeat(np.arange(EXPERTS), np.array(load_profile()))

    def one_micro(micro_key):
        sub_keys = jax.random.split(micro_key)
        expert_of_rank = jax.random.permutation(sub_keys[0], EXPERTS)
        id_grid = expert_of_rank[rank_ids].reshape(TOP, TOKENS).T
        device_keys = jax.random.split(sub_keys[1], GROUP)

        def one_device(device_key):
            return id_grid[jax.random.permutation(device_key, TOKENS)]

        return jax.vmap(one_device)(device_keys).reshape(GROUP * TOKENS, TOP)

    return jax.vmap(one_micro)(jax.random.split(base_key, 2)).astype(jnp.int32)


def draw_normal(sub_key, array_shape, std_scale):
    return (jax.random.normal(sub_key, array_shape, jnp.float32) * std_scale).astype(jnp.bfloat16)


def setup_inputs(seed: int = 0, part: int = 0) -> dict:
    weight_keys = jax.random.split(jax.random.key(seed), 12)
    part_keys = jax.random.split(jax.random.fold_in(jax.random.key(seed + 1), part), 3)
    n_rows = GROUP * TOKENS
    attn_width = HEADS * HEAD_DIM
    return {
        "tokens": draw_normal(part_keys[0], (2, n_rows // SEQ, SEQ, D_MODEL), 1.0),
        "expert_ids": draw_routing(part_keys[1]),
        "route_weights": jax.nn.softmax(jax.random.normal(part_keys[2], (2, n_rows, TOP), jnp.float32), axis=-1),
        "attn_norm": jax.random.uniform(weight_keys[0], (D_MODEL,), jnp.float32, 0.5, 1.5).astype(jnp.bfloat16),
        "w_query": draw_normal(weight_keys[1], (D_MODEL, HEADS, HEAD_DIM), D_MODEL ** -0.5),
        "w_key": draw_normal(weight_keys[2], (D_MODEL, HEADS, HEAD_DIM), D_MODEL ** -0.5),
        "w_value": draw_normal(weight_keys[3], (D_MODEL, HEADS, HEAD_DIM), D_MODEL ** -0.5),
        "w_out": draw_normal(weight_keys[4], (HEADS, HEAD_DIM, D_MODEL), attn_width ** -0.5),
        "ffn_norm": jax.random.uniform(weight_keys[5], (D_MODEL,), jnp.float32, 0.5, 1.5).astype(jnp.bfloat16),
        "w_gate": draw_normal(weight_keys[6], (EXPERTS, D_MODEL, FF), D_MODEL ** -0.5),
        "w_up": draw_normal(weight_keys[7], (EXPERTS, D_MODEL, FF), D_MODEL ** -0.5),
        "w_down": draw_normal(weight_keys[8], (EXPERTS, FF, D_MODEL), 2.0 * FF ** -0.5),
        "shared_gate": draw_normal(weight_keys[9], (D_MODEL, SHARED_FF), D_MODEL ** -0.5),
        "shared_up": draw_normal(weight_keys[10], (D_MODEL, SHARED_FF), D_MODEL ** -0.5),
        "shared_down": draw_normal(weight_keys[11], (SHARED_FF, D_MODEL), SHARED_FF ** -0.5),
    }


def rms_norm(in_vals, norm_gain):
    wide_vals = in_vals.astype(jnp.float32)
    inv_rms = lax.rsqrt(jnp.mean(wide_vals * wide_vals, axis=-1, keepdims=True) + NORM_EPS)
    return (wide_vals * inv_rms * norm_gain.astype(jnp.float32)).astype(jnp.bfloat16)


def attention_block(seq_rows, attn_norm, w_query, w_key, w_value, w_out):
    n_seq = seq_rows.shape[0]
    normed = rms_norm(seq_rows, attn_norm).reshape(n_seq * SEQ, D_MODEL)

    def project(weight):
        proj_rows = jnp.dot(normed, weight.reshape(D_MODEL, HEADS * HEAD_DIM), preferred_element_type=jnp.float32)
        return proj_rows.astype(jnp.bfloat16).reshape(n_seq, SEQ, HEADS, HEAD_DIM)

    queries = project(w_query)
    key_rows = project(w_key)
    value_rows = project(w_value)
    scores = jnp.einsum("bqhe,bkhe->bhqk", queries.astype(jnp.float32), key_rows.astype(jnp.float32)) * HEAD_DIM ** -0.5
    causal = jnp.arange(SEQ)[:, None] >= jnp.arange(SEQ)[None, :]
    attn_probs = jax.nn.softmax(jnp.where(causal, scores, -jnp.inf), axis=-1).astype(jnp.bfloat16)
    head_mix = jnp.einsum("bhqk,bkhe->bqhe", attn_probs.astype(jnp.float32), value_rows.astype(jnp.float32)).astype(jnp.bfloat16)
    attn_out = jnp.dot(head_mix.reshape(n_seq * SEQ, HEADS * HEAD_DIM), w_out.reshape(HEADS * HEAD_DIM, D_MODEL), preferred_element_type=jnp.float32)
    return (seq_rows.astype(jnp.float32) + attn_out.reshape(n_seq, SEQ, D_MODEL)).astype(jnp.bfloat16)


def swiglu(in_rows, gate_w, up_w, down_w):
    gate_act = jnp.dot(in_rows, gate_w, preferred_element_type=jnp.float32)
    up_act = jnp.dot(in_rows, up_w, preferred_element_type=jnp.float32)
    hidden = (jax.nn.silu(gate_act) * up_act).astype(jnp.bfloat16)
    return jnp.dot(hidden, down_w, preferred_element_type=jnp.float32).astype(jnp.bfloat16)


def route_plan(flat_ids, slot_cap):
    n_rows = flat_ids.shape[0]
    sort_order = jnp.argsort(flat_ids, stable=True).astype(jnp.int32)
    counts = jnp.bincount(flat_ids, length=EXPERTS)
    starts = jnp.cumsum(counts) - counts
    sorted_rank = jnp.zeros((n_rows,), jnp.int32).at[sort_order].set(jnp.arange(n_rows, dtype=jnp.int32))
    slot_ids = sorted_rank - starts[flat_ids]
    src_pos = sort_order[jnp.minimum(starts[:, None] + jnp.arange(slot_cap)[None, :], n_rows - 1)]
    return slot_ids, src_pos


def reference(tokens, expert_ids, route_weights, attn_norm, w_query, w_key, w_value, w_out, ffn_norm, w_gate, w_up, w_down, shared_gate, shared_up, shared_down):
    def one_micro(micro_inputs):
        micro_tok, micro_ids, micro_weights = micro_inputs
        dev_seqs = micro_tok.reshape(GROUP, TOKENS // SEQ, SEQ, D_MODEL)
        residual = lax.map(lambda dev_rows: attention_block(dev_rows, attn_norm, w_query, w_key, w_value, w_out), dev_seqs)
        residual = residual.reshape(GROUP * TOKENS, D_MODEL)
        normed = rms_norm(residual, ffn_norm)
        shared_out = swiglu(normed, shared_gate, shared_up, shared_down)
        flat_ids = micro_ids.reshape(-1)
        slot_cap = GROUP * CAPACITY
        slot_ids, src_pos = route_plan(flat_ids, slot_cap)
        expert_in = normed[src_pos // TOP]
        expert_out = lax.map(lambda packed: swiglu(packed[0], packed[1], packed[2], packed[3]), (expert_in, w_gate, w_up, w_down))
        picked = expert_out.reshape(EXPERTS * slot_cap, D_MODEL)[flat_ids * slot_cap + slot_ids]
        picked = picked.reshape(GROUP * TOKENS, TOP, D_MODEL)
        routed = jnp.sum(picked.astype(jnp.float32) * micro_weights[:, :, None], axis=1)
        layer_rows = residual.astype(jnp.float32) + shared_out.astype(jnp.float32) + routed
        return layer_rows.astype(jnp.bfloat16).reshape(micro_tok.shape)

    return lax.map(one_micro, (tokens, expert_ids, route_weights))
```

```python
import functools

import jax
import jax.numpy as jnp
from jax import lax
from jax.experimental import pallas as pl
from jax.experimental.pallas import tpu as pltpu
from jax.sharding import PartitionSpec as P

NORM_EPS = 1e-6
CHUNKS = 2


def rms_norm(in_vals, norm_gain):
    wide_vals = in_vals.astype(jnp.float32)
    inv_rms = lax.rsqrt(jnp.mean(wide_vals * wide_vals, axis=-1, keepdims=True) + NORM_EPS)
    return (wide_vals * inv_rms * norm_gain.astype(jnp.float32)).astype(jnp.bfloat16)


def attention_block(seq_rows, attn_norm, w_query, w_key, w_value, w_out):
    normed = rms_norm(seq_rows, attn_norm)
    queries = jnp.einsum("...sd,dhe->...she", normed, w_query, preferred_element_type=jnp.float32).astype(jnp.bfloat16)
    key_rows = jnp.einsum("...sd,dhe->...she", normed, w_key, preferred_element_type=jnp.float32).astype(jnp.bfloat16)
    value_rows = jnp.einsum("...sd,dhe->...she", normed, w_value, preferred_element_type=jnp.float32).astype(jnp.bfloat16)
    seq_len = seq_rows.shape[-2]
    scores = jnp.einsum("...qhe,...khe->...hqk", queries, key_rows, preferred_element_type=jnp.float32) * (w_query.shape[-1] ** -0.5)
    causal = jnp.arange(seq_len)[:, None] >= jnp.arange(seq_len)[None, :]
    attn_probs = jax.nn.softmax(jnp.where(causal, scores, -jnp.inf), axis=-1).astype(jnp.bfloat16)
    head_mix = jnp.einsum("...hqk,...khe->...qhe", attn_probs, value_rows, preferred_element_type=jnp.float32).astype(jnp.bfloat16)
    attn_out = jnp.einsum("...qhe,hed->...qd", head_mix, w_out, preferred_element_type=jnp.float32)
    return (seq_rows.astype(jnp.float32) + attn_out).astype(jnp.bfloat16)


def swiglu(in_rows, gate_w, up_w, down_w):
    gate_act = jnp.dot(in_rows, gate_w, preferred_element_type=jnp.float32)
    up_act = jnp.dot(in_rows, up_w, preferred_element_type=jnp.float32)
    hidden = (jax.nn.silu(gate_act) * up_act).astype(jnp.bfloat16)
    return jnp.dot(hidden, down_w, preferred_element_type=jnp.float32).astype(jnp.bfloat16)


def expert_body(z_ref, w_ref, gate_ref, up_ref, down_ref, out_ref):
    rows = z_ref.shape[0] * z_ref.shape[1]
    z_rows = z_ref[...].reshape(rows, z_ref.shape[2])
    w_rows = w_ref[...].reshape(rows, w_ref.shape[2])
    for e in range(gate_ref.shape[0]):
        gate_act = jnp.dot(z_rows, gate_ref[e], preferred_element_type=jnp.float32)
        up_act = jnp.dot(z_rows, up_ref[e], preferred_element_type=jnp.float32)
        hidden = (jax.nn.silu(gate_act) * up_act).astype(jnp.bfloat16)
        rows_out = jnp.dot(hidden, down_ref[e], preferred_element_type=jnp.float32).astype(jnp.bfloat16)
        w_col = w_rows[:, e : e + 1]
        term = jnp.where(w_col > 0, rows_out.astype(jnp.float32) * w_col, 0.0)
        term = term.reshape(out_ref.shape)
        if e == 0:
            out_ref[...] = term
        else:
            out_ref[...] += term


def expert_sums(z_all, w_all, w_gate, w_up, w_down, part, parts):
    n_src, n_tok, d_model = z_all.shape
    local = w_gate.shape[0]
    ff = w_gate.shape[2]
    rows = n_tok // parts
    srcs = parts
    flops = 6 * n_src * rows * d_model * ff * local
    return pl.pallas_call(
        expert_body,
        grid=(n_src // srcs,),
        out_shape=jax.ShapeDtypeStruct((n_src, rows, d_model), jnp.float32),
        in_specs=[
            pl.BlockSpec((srcs, rows, d_model), lambda i: (i, part, 0)),
            pl.BlockSpec((srcs, rows, local), lambda i: (i, part, 0)),
            pl.BlockSpec((local, d_model, ff), lambda i: (0, 0, 0), pipeline_mode=pl.Buffered(1)),
            pl.BlockSpec((local, d_model, ff), lambda i: (0, 0, 0), pipeline_mode=pl.Buffered(1)),
            pl.BlockSpec((local, ff, d_model), lambda i: (0, 0, 0), pipeline_mode=pl.Buffered(1)),
        ],
        out_specs=pl.BlockSpec((srcs, rows, d_model), lambda i: (i, 0, 0)),
        compiler_params=pltpu.CompilerParams(vmem_limit_bytes=52 * 1024 * 1024),
        cost_estimate=pl.CostEstimate(flops=flops, bytes_accessed=n_src * rows * d_model * 6, transcendentals=n_src * rows * ff * local),
        name="expert_sums",
    )(z_all, w_all, w_gate, w_up, w_down)


def solution(mesh):
    group_size = mesh.shape["ep"]

    def device_step(tokens, expert_ids, route_weights, attn_norm, w_query, w_key, w_value, w_out, ffn_norm, w_gate, w_up, w_down, shared_gate, shared_up, shared_down):
        n_micro, n_seq, seq_len, d_model = tokens.shape
        n_tok = n_seq * seq_len
        local_experts = w_gate.shape[0]
        experts = local_experts * group_size
        me = lax.axis_index("ep")
        hot = expert_ids[..., None] == jnp.arange(experts, dtype=jnp.int32)
        dense_w = jnp.sum(jnp.where(hot, route_weights[..., None], 0.0), axis=2)
        all_w = lax.all_gather(dense_w, "ep")
        my_w = lax.dynamic_slice_in_dim(all_w, me * local_experts, local_experts, axis=3)
        residuals, norms, gathered = [], [], []
        for m in range(n_micro):
            residual = attention_block(tokens[m], attn_norm, w_query, w_key, w_value, w_out).reshape(n_tok, d_model)
            normed = rms_norm(residual, ffn_norm)
            residuals.append(residual)
            norms.append(normed)
            gathered.append(lax.all_gather(normed, "ep"))
        micro_outs = []
        for m in range(n_micro):
            shared_out = swiglu(norms[m], shared_gate, shared_up, shared_down)
            pieces = []
            for c in range(CHUNKS):
                sums = expert_sums(gathered[m], my_w[:, m], w_gate, w_up, w_down, c, CHUNKS)
                pieces.append(lax.psum_scatter(sums, "ep", scatter_dimension=0))
            routed = jnp.concatenate(pieces, axis=0)
            layer_rows = residuals[m].astype(jnp.float32) + shared_out.astype(jnp.float32) + routed
            micro_outs.append(layer_rows.astype(jnp.bfloat16).reshape(n_seq, seq_len, d_model))
        return jnp.stack(micro_outs)

    token_spec = P(None, ("dp", "ep"), None, None)
    route_spec = P(None, ("dp", "ep"), None)
    rep_spec = P()
    expert_spec = P("ep", None, None)
    in_specs = (token_spec, route_spec, route_spec, rep_spec, rep_spec, rep_spec, rep_spec, rep_spec, rep_spec, expert_spec, expert_spec, expert_spec, rep_spec, rep_spec, rep_spec)
    return jax.shard_map(device_step, mesh=mesh, in_specs=in_specs, out_specs=token_spec, check_vma=False)
```
